32 devices in a mesh: trade: 4 (over z), node: 8 (over y, x, core).
Axes of the slice: x: 2, y: 2, z: 4, core: 2. Of those that a mesh axis runs over, the one named last changes fastest.
Arguments:
- values_in: float32 [1024, 16384], P('trade', 'node'), may hold values from 0 to 1
- prob_up: float32 [16, 16384], P(None, 'node'), may hold values from 0.1 to 0.3
- prob_down: float32 [16, 16384], P(None, 'node'), may hold values from 0.1 to 0.3
- discount: float32 [16, 16384], P(None, 'node'), may hold values from 0.9 to 1
- swap_rate: float32 [16, 16384], P(None, 'node'), may hold values from -3 to 3
- annuity: float32 [16, 16384], P(None, 'node'), may hold values from 0.5 to 2
- state_price: float32 [16384], P('node'), may hold values from 3.0517578e-05 to 0.00012207031
- exercise_step: int32 [1024, 4], P('trade'), may hold values from 0 to 15
- strike_bucket: int32 [1024], P('trade'), may hold values from 0 to 63
- notional_sign: int32 [1024], P('trade'), may hold values from 0 to 1
- strike_table: float32 [64], replicated, may hold values from -0.5 to 0.5
Outputs:
- values_out: float32 [1024, 16384], P(('trade', 'node'))
- prices: float32 [1024], P(('trade', 'node'))
- portfolio: float32 [], replicated
The draws below stay inside these ranges and needn't reach their ends.
All inputs are finite; a program needn't handle non-finite values.
Results may differ from the reference program's by a relative error of at most 0.0003.
Values sent between devices are 32-bit elements; how exact they have to be, the bound alone decides.
A program may use at most 128 MiB of HBM per device.

```python
import math
import jax
import jax.numpy as jnp
from jax import lax

TRADE_DEV = 256
STEPS = 16
EXDATES = 4
BUCKETS = 64
NODES = 16384
TRADES = 1024
N_TRADE = 4


def touch_ends(drawn, stream_key, low, top_value):
    shape = drawn.shape
    index_at = [jax.random.randint(jax.random.fold_in(stream_key, axis), (), 0, shape[axis]) for axis in range(len(shape))]
    drawn = drawn.at[tuple(index_at)].set(low)
    longest = shape.index(max(shape))
    index_at[longest] = (index_at[longest] + 1) % shape[longest]
    return drawn.at[tuple(index_at)].set(top_value)


def block_levels(rng, shape, cuts, least, largest):
    level, own = 1.0, jax.random.fold_in(rng, 6)
    for axis_at, shards_of in cuts:
        heights = jnp.exp(jax.random.uniform(jax.random.fold_in(own, axis_at), (shards_of,), jnp.float32, least / len(cuts), largest / len(cuts)))
        level = level * jnp.repeat(heights, shape[axis_at] // shards_of).reshape([-1 if axis == axis_at else 1 for axis in range(len(shape))])
    return level


def normal_values(own_key, dims, deviation, most, cuts=(), held_as=jnp.bfloat16):
    entries = jax.random.normal(own_key, dims, jnp.float32) * deviation
    if len(cuts) > 0:
        entries = block_levels(own_key, dims, cuts, -0.22, 0.18) * entries
    return jnp.clip(entries, min=-most, max=most).astype(held_as)


def setup_inputs(seed: int = 0) -> dict:
    arg_keys = jax.random.split(jax.random.key(seed), 12)
    values_in = jnp.clip(1.0 * jax.random.uniform(arg_keys[0], (TRADES, NODES), jnp.float32) ** block_levels(arg_keys[0], (TRADES, NODES), ((0, 4), (1, 8)), -0.2, 0.2), 0.0, 1.0)
    prob_up = jnp.clip(0.1 + 0.20000001043081284 * jax.random.uniform(arg_keys[1], (STEPS, NODES), jnp.float32) ** block_levels(arg_keys[1], (STEPS, NODES), ((1, 8),), -0.2, 0.2), 0.1, 0.3)
    prob_down = jnp.clip(0.1 + 0.20000001043081284 * jax.random.uniform(arg_keys[2], (STEPS, NODES), jnp.float32) ** block_levels(arg_keys[2], (STEPS, NODES), ((1, 8),), -0.2, 0.2), 0.1, 0.3)
    discount = jnp.clip(0.9 + 0.100000024 * jax.random.uniform(arg_keys[3], (STEPS, NODES), jnp.float32) ** block_levels(arg_keys[3], (STEPS, NODES), ((1, 8),), -0.2, 0.2), 0.9, 1.0)
    swap_rate = normal_values(arg_keys[4], (STEPS, NODES), 0.5, 3.0, ((1, 8),), jnp.float32)
    annuity = jnp.clip(jnp.exp(math.log(2.0) - 1.3862944 * jax.random.uniform(arg_keys[5], (STEPS, NODES), jnp.float32) ** block_levels(arg_keys[5], (STEPS, NODES), ((1, 8),), -0.2, 0.2)), 0.5, 2.0)
    state_price = jnp.clip(jnp.exp(math.log(0.00012207031) - 1.3862944 * jax.random.uniform(arg_keys[6], (NODES,), jnp.float32) ** block_levels(arg_keys[6], (NODES,), ((0, 8),), -0.2, 0.2)), 3.0517578125e-05, 0.00012207031)
    exercise_step = touch_ends(jax.random.randint(arg_keys[7], (TRADES, EXDATES), 0, STEPS), jax.random.fold_in(arg_keys[7], 1), 0, STEPS - 1).astype(jnp.int32)
    strike_bucket = touch_ends(jax.random.randint(arg_keys[8], (TRADES,), 0, BUCKETS), jax.random.fold_in(arg_keys[8], 1), 0, BUCKETS - 1).astype(jnp.int32)
    notional_sign = touch_ends(jax.random.randint(arg_keys[9], (TRADES,), 0, 2), jax.random.fold_in(arg_keys[9], 1), 0, 1).astype(jnp.int32)
    strike_table = jnp.clip(jax.random.uniform(arg_keys[10], (BUCKETS,), jnp.float32, -0.5, 0.5), -0.5, 0.5)
    return {"values_in": values_in, "prob_up": prob_up, "prob_down": prob_down, "discount": discount, "swap_rate": swap_rate, "annuity": annuity, "state_price": state_price, "exercise_step": exercise_step, "strike_bucket": strike_bucket, "notional_sign": notional_sign, "strike_table": strike_table}


def strikes_of(bucket, strike_table):
    levels = lax.broadcasted_iota(jnp.int32, (1, strike_table.shape[0]), 1)
    return jnp.sum(jnp.where(bucket[:, None] == levels, strike_table[None, :], jnp.zeros((), strike_table.dtype)), axis=1)


def roll_once(padded, prob_up, prob_down, discount_row):
    middle = 1.0 - prob_up - prob_down
    return discount_row * (prob_up * padded[:, 2:] + middle * padded[:, 1:-1] + prob_down * padded[:, :-2])


def exercise(values, active, strike, signs, swap_row, annuity_row):
    payoff = signs[:, None] * annuity_row[None, :] * (swap_row[None, :] - strike[:, None])
    return jnp.where(active[:, None], jnp.maximum(values, payoff), values)


def reference(values_in, prob_up, prob_down, discount, swap_rate, annuity, state_price, exercise_step, strike_bucket, notional_sign, strike_table):
    strike = strikes_of(strike_bucket, strike_table)
    signs = (2 * notional_sign - 1).astype(jnp.float32)

    def one_block(pieces):
        values, dates, strikes, sign_rows = pieces
        for step in range(STEPS):
            padded = jnp.pad(values, ((0, 0), (1, 1)))
            values = roll_once(padded, prob_up[step], prob_down[step], discount[step])
            active = jnp.any(dates == step, axis=1)
            values = exercise(values, active, strikes, sign_rows, swap_rate[step], annuity[step])
        block_prices = jnp.sum(values * state_price[None, :], axis=1)
        return values, block_prices

    shaped = (values_in.reshape(N_TRADE, TRADE_DEV, NODES), exercise_step.reshape(N_TRADE, TRADE_DEV, EXDATES), strike.reshape(N_TRADE, TRADE_DEV), signs.reshape(N_TRADE, TRADE_DEV))
    values_all, prices_all = lax.map(one_block, shaped)
    prices = prices_all.reshape(TRADES)
    portfolio = jnp.sum(prices) / TRADE_DEV
    return values_all.reshape(TRADES, NODES), prices, portfolio
```

```python
import functools

import jax
import jax.numpy as jnp
from jax import lax
from jax.experimental import pallas as pl
from jax.experimental.pallas import tpu as pltpu
from jax.sharding import PartitionSpec as P

MESH = pl.DeviceIdType.MESH
LANES = 128
SUB = 8


def kernel(
    node_count,
    trade_count,
    values_hbm,
    up_hbm,
    down_hbm,
    disc_hbm,
    swap_hbm,
    ann_hbm,
    price_ref,
    dates_ref,
    bucket_ref,
    sign_ref,
    table_ref,
    out_ref,
    small_ref,
    work,
    lattice,
    halo_values,
    halo_lattice,
    coef,
    rows_t,
    sign_b,
    strike_b,
    dates_b,
    z_send,
    z_recv,
    msg_send,
    msg_recv,
    in_sem,
    lat_sem,
    self_sem,
    hv_send,
    hv_recv,
    hl_send,
    hl_recv,
    block_send,
    block_recv,
    zs_sem,
    zr_sem,
    ms_sem,
    mr_sem,
):
    n = node_count
    me = lax.axis_index("node")
    my_trade = lax.axis_index("trade")
    trades, width = values_hbm.shape
    steps = up_hbm.shape[0]
    rows = trades // n
    cols = width // LANES
    tiles = 2 if rows % (2 * SUB) == 0 else 1
    group_rows = tiles * SUB
    lat_hbm = (up_hbm, down_hbm, disc_hbm, swap_hbm, ann_hbm)

    def peer(turn):
        mask = n - 1 - turn
        if n & (n - 1):
            return lax.rem(mask + n - me + n, n)
        total, bit = 0, 1
        while bit < n:
            total = total + lax.rem(me // bit + mask // bit, 2) * bit
            bit *= 2
        return total

    def in_copy(turn):
        at = pl.ds(pl.multiple_of(peer(turn) * rows, SUB), rows)
        return pltpu.make_async_copy(values_hbm.at[at], work.at[at], in_sem.at[turn])

    lat_copies = [
        pltpu.make_async_copy(lat_hbm[i], lattice.at[i], lat_sem.at[i]) for i in range(5)
    ]
    for copy in lat_copies:
        copy.start()
    for turn in range(n):
        in_copy(turn).start()

    barrier = pltpu.get_barrier_semaphore()
    for k in range(1, n):
        pl.semaphore_signal(
            barrier, inc=1, device_id={"node": lax.rem(me + k, n)}, device_id_type=MESH
        )
    for k in range(1, trade_count):
        pl.semaphore_signal(
            barrier,
            inc=1,
            device_id={"trade": lax.rem(my_trade + k, trade_count)},
            device_id_type=MESH,
        )
    pl.semaphore_wait(barrier, n - 1 + trade_count - 1)

    right, left = lax.rem(me + 1, n), lax.rem(me + n - 1, n)
    first, last = pl.ds(0, LANES), pl.ds(width - LANES, LANES)
    halos = []
    for side, (target, edge) in enumerate(((right, last), (left, first))):
        for i in range(5):
            halos.append(
                pltpu.make_async_remote_copy(
                    src_ref=lat_hbm[i].at[:, edge],
                    dst_ref=halo_lattice.at[side, i],
                    send_sem=hl_send.at[side, i],
                    recv_sem=hl_recv.at[side, i],
                    device_id={"node": target},
                    device_id_type=MESH,
                )
            )
        halos.append(
            pltpu.make_async_remote_copy(
                src_ref=values_hbm.at[:, edge],
                dst_ref=halo_values.at[side],
                send_sem=hv_send.at[side],
                recv_sem=hv_recv.at[side],
                device_id={"node": target},
                device_id_type=MESH,
            )
        )
    for copy in halos:
        copy.start()

    rows_t[0:4, :] = dates_ref[...].astype(jnp.float32)
    rows_t[4:5, :] = bucket_ref[...].astype(jnp.float32)
    rows_t[5:6, :] = sign_ref[...].astype(jnp.float32)
    rows_t[6:8, :] = jnp.zeros((2, trades), jnp.float32)
    per_trade = rows_t[...].T
    levels = lax.broadcasted_iota(jnp.int32, (trades, table_ref.shape[1]), 1).astype(jnp.float32)
    strike = jnp.sum(
        jnp.where(per_trade[:, 4:5] == levels, table_ref[...], 0.0), axis=1, keepdims=True
    )
    sign = 2.0 * per_trade[:, 5:6] - 1.0
    sign_b[...] = jnp.broadcast_to(sign, (trades, LANES))
    strike_b[...] = jnp.broadcast_to(sign * strike, (trades, LANES))
    for e in range(4):
        dates_b[e] = jnp.broadcast_to(per_trade[:, e : e + 1], (trades, LANES))

    for copy in lat_copies:
        copy.wait()

    def widen(row):
        return jnp.broadcast_to(row, (SUB, LANES))

    def spread(first_step, k, up, down, disc, swap, ann):
        rows_of = (disc * up, disc * (1.0 - up - down), disc * down, ann * swap, ann)
        for i, block in enumerate(rows_of):
            for r in range(SUB):
                coef[i, first_step + r, k] = widen(block[r : r + 1])

    def prepare(k, carry):
        at = pl.ds(pl.multiple_of(k * LANES, LANES), LANES)
        for first_step in range(0, steps, SUB):
            spread(
                first_step, k, *[lattice[i, pl.ds(first_step, SUB), at] for i in range(5)]
            )
        return carry

    lax.fori_loop(0, cols, prepare, 0)

    lane = lax.broadcasted_iota(jnp.int32, (SUB, LANES), 1)
    row = lax.broadcasted_iota(jnp.int32, (SUB, LANES), 0)
    on_right = lane < LANES // 2
    has_right = jnp.where(me < n - 1, 1.0, 0.0)
    has_left = jnp.where(me > 0, 1.0, 0.0)
    inside = jnp.where(lane < steps, has_right, jnp.where(lane >= LANES - steps, has_left, 0.0))

    for copy in halos:
        copy.wait()

    for first_step in range(0, steps, SUB):
        at = pl.ds(first_step, SUB)
        up, down, disc, swap, ann = [
            jnp.where(on_right, halo_lattice[1, i, at, :], halo_lattice[0, i, at, :])
            for i in range(5)
        ]
        spread(first_step, cols, up, down, disc * inside, swap, ann * inside)

    is_first, is_last = lane == 0, lane == LANES - 1
    count = cols + 1

    def group(base, offset, total, message):
        parts = []
        for u in range(tiles):
            at = pl.ds(pl.multiple_of(base + u * SUB, SUB), SUB)
            held = [work[at, pl.ds(k * LANES, LANES)] for k in range(cols)]
            held.append(
                inside * jnp.where(on_right, halo_values[1, at, :], halo_values[0, at, :])
            )
            parts.append(held)
        dates = [
            [
                dates_b[e, pl.ds(pl.multiple_of(base + u * SUB, SUB), SUB), :]
                for e in range(4)
            ]
            for u in range(tiles)
        ]
        signs = [
            sign_b[pl.ds(pl.multiple_of(base + u * SUB, SUB), SUB), :] for u in range(tiles)
        ]
        strikes = [
            strike_b[pl.ds(pl.multiple_of(base + u * SUB, SUB), SUB), :] for u in range(tiles)
        ]

        def step_once(step, flat):
            now = step.astype(jnp.float32)
            scale, shift = [], []
            for u in range(tiles):
                d = dates[u]
                active = (d[0] == now) | (d[1] == now) | (d[2] == now) | (d[3] == now)
                scale.append(jnp.where(active, signs[u], 0.0))
                shift.append(jnp.where(active, strikes[u], 0.0))
            old = [flat[u * count : (u + 1) * count] for u in range(tiles)]
            down = [[pltpu.roll(x, 1, 1) for x in old[u]] for u in range(tiles)]
            up = [[pltpu.roll(x, LANES - 1, 1) for x in old[u]] for u in range(tiles)]
            new = [[] for _ in range(tiles)]
            for k in range(count):
                a, b, c = coef[0, step, k], coef[1, step, k], coef[2, step, k]
                pay, ann = coef[3, step, k], coef[4, step, k]
                for u in range(tiles):
                    above = jnp.where(is_last, up[u][(k + 1) % count], up[u][k])
                    below = jnp.where(is_first, down[u][k - 1], down[u][k])
                    rolled = a * above + b * old[u][k] + c * below
                    new[u].append(jnp.maximum(rolled, scale[u] * pay - shift[u] * ann))
            return tuple(x for u in range(tiles) for x in new[u])

        flat = lax.fori_loop(0, steps, step_once, tuple(x for held in parts for x in held))
        for u in range(tiles):
            at = pl.ds(pl.multiple_of(base + u * SUB, SUB), SUB)
            priced = jnp.zeros((SUB, LANES), jnp.float32)
            for k in range(cols):
                x = flat[u * count + k]
                work[at, pl.ds(k * LANES, LANES)] = x
                priced = priced + x * widen(price_ref[:, pl.ds(k * LANES, LANES)])
            total = total + priced
            summed = jnp.sum(priced, axis=1, keepdims=True)
            message = message + jnp.where(lane == offset + u * SUB + row, summed, 0.0)
        return total, message

    my_cols = pl.ds(pl.multiple_of(me * width, LANES), width)

    def block_copy(turn):
        target = peer(turn)
        return pltpu.make_async_remote_copy(
            src_ref=work.at[pl.ds(pl.multiple_of(target * rows, SUB), rows)],
            dst_ref=out_ref.at[:, my_cols],
            send_sem=block_send.at[turn],
            recv_sem=block_recv.at[turn],
            device_id={"node": target},
            device_id_type=MESH,
        )

    zero = jnp.zeros((SUB, LANES), jnp.float32)

    def chunk(turn, total):
        start = peer(turn) * rows
        in_copy(turn).wait()

        def one(g, carry):
            return group(start + g * group_rows, g * group_rows, *carry)

        total, message = lax.fori_loop(0, rows // group_rows, one, (total, zero))
        msg_send[turn] = message

        @pl.when(turn < n - 1)
        def _():
            block_copy(turn).start()

        return total

    total = lax.fori_loop(0, n, chunk, zero)
    own = pltpu.make_async_copy(
        work.at[pl.ds(pl.multiple_of(me * rows, SUB), rows)], out_ref.at[:, my_cols], self_sem
    )
    own.start()

    z_send[...] = total
    z_copies = [
        pltpu.make_async_remote_copy(
            src_ref=z_send,
            dst_ref=z_recv.at[k - 1],
            send_sem=zs_sem.at[k - 1],
            recv_sem=zr_sem.at[k - 1],
            device_id={"trade": lax.rem(my_trade + k, trade_count)},
            device_id_type=MESH,
        )
        for k in range(1, trade_count)
    ]
    for copy in z_copies:
        copy.start()
    for k, copy in enumerate(z_copies):
        copy.wait()
        total = total + z_recv[k]
    summed = jnp.where(lane == LANES - 1, jnp.sum(total, axis=1, keepdims=True), 0.0)
    for turn in range(n):
        msg_send[turn] = msg_send[turn] + summed

    def msg_copy(turn):
        return pltpu.make_async_remote_copy(
            src_ref=msg_send.at[turn],
            dst_ref=msg_recv.at[turn],
            send_sem=ms_sem.at[turn],
            recv_sem=mr_sem.at[turn],
            device_id={"node": peer(turn)},
            device_id_type=MESH,
        )

    own.wait()
    for turn in range(n - 1):
        msg_copy(turn).start()
    result = msg_send[n - 1]
    for turn in range(n - 1):
        msg_copy(turn).wait()
        result = result + msg_recv[turn]
    small_ref[...] = jnp.sum(result, axis=0, keepdims=True)
    for turn in range(n - 1):
        block_copy(turn).wait()


def local(
    node_count,
    trade_count,
    values_in,
    prob_up,
    prob_down,
    discount,
    swap_rate,
    annuity,
    state_price,
    exercise_step,
    strike_bucket,
    notional_sign,
    strike_table,
):
    trades, width = values_in.shape
    steps = prob_up.shape[0]
    n = node_count
    rows = trades // n
    f32 = jnp.float32
    dma = pltpu.SemaphoreType.DMA
    any_spec = pl.BlockSpec(memory_space=pl.ANY)
    vmem_spec = pl.BlockSpec(memory_space=pltpu.VMEM)
    values, small = pl.pallas_call(
        functools.partial(kernel, n, trade_count),
        out_shape=(
            jax.ShapeDtypeStruct((rows, width * n), f32),
            jax.ShapeDtypeStruct((1, LANES), f32),
        ),
        in_specs=[any_spec] * 6 + [vmem_spec] * 5,
        out_specs=(vmem_spec, vmem_spec),
        scratch_shapes=[
            pltpu.VMEM((trades, width), f32),
            pltpu.VMEM((5, steps, width), f32),
            pltpu.VMEM((2, trades, LANES), f32),
            pltpu.VMEM((2, 5, steps, LANES), f32),
            pltpu.VMEM((5, steps, width // LANES + 1, SUB, LANES), f32),
            pltpu.VMEM((SUB, trades), f32),
            pltpu.VMEM((trades, LANES), f32),
            pltpu.VMEM((trades, LANES), f32),
            pltpu.VMEM((4, trades, LANES), f32),
            pltpu.VMEM((SUB, LANES), f32),
            pltpu.VMEM((trade_count - 1, SUB, LANES), f32),
            pltpu.VMEM((n, SUB, LANES), f32),
            pltpu.VMEM((n - 1, SUB, LANES), f32),
            dma((n,)),
            dma((5,)),
            dma,
            dma((2,)),
            dma((2,)),
            dma((2, 5)),
            dma((2, 5)),
            dma((n - 1,)),
            dma((n - 1,)),
            dma((trade_count - 1,)),
            dma((trade_count - 1,)),
            dma((n - 1,)),
            dma((n - 1,)),
        ],
        compiler_params=pltpu.CompilerParams(
            collective_id=0, has_side_effects=True, vmem_limit_bytes=32 * 1024 * 1024
        ),
    )(
        values_in,
        prob_up,
        prob_down,
        discount,
        swap_rate,
        annuity,
        state_price.reshape(1, width),
        exercise_step.T,
        strike_bucket.reshape(1, trades),
        notional_sign.reshape(1, trades),
        strike_table.reshape(1, strike_table.shape[0]),
    )
    return (values, small[0, :rows], small[0, LANES - 1] / trades)


def solution(mesh):
    in_specs = (
        P("trade", "node"),
        P(None, "node"),
        P(None, "node"),
        P(None, "node"),
        P(None, "node"),
        P(None, "node"),
        P("node"),
        P("trade", None),
        P("trade"),
        P("trade"),
        P(),
    )
    out_specs = (P(("trade", "node"), None), P(("trade", "node")), P())
    body = functools.partial(local, mesh.shape["node"], mesh.shape["trade"])
    return jax.shard_map(body, mesh=mesh, in_specs=in_specs, out_specs=out_specs, check_vma=False)
```

```python
import functools

import jax
import jax.numpy as jnp
from jax import lax
from jax.experimental import pallas as pl
from jax.experimental.pallas import tpu as pltpu
from jax.sharding import PartitionSpec as P

MESH = pl.DeviceIdType.MESH
LANES = 128
SUB = 8


def kernel(
    node_count,
    trade_count,
    values_hbm,
    up_hbm,
    down_hbm,
    disc_hbm,
    swap_hbm,
    ann_hbm,
    price_hbm,
    dates_hbm,
    bucket_hbm,
    sign_hbm,
    table_hbm,
    out_ref,
    small_ref,
    work,
    lattice,
    price_ref,
    dates_ref,
    bucket_ref,
    sign_ref,
    table_ref,
    halo_values,
    halo_lattice,
    coef,
    rows_t,
    sign_b,
    strike_b,
    dates_b,
    z_send,
    z_recv,
    msg_send,
    msg_recv,
    in_sem,
    lat_sem,
    trade_sem,
    self_sem,
    hv_send,
    hv_recv,
    hl_send,
    hl_recv,
    block_send,
    block_recv,
    zs_sem,
    zr_sem,
    ms_sem,
    mr_sem,
):
    n = node_count
    me = lax.axis_index("node")
    my_trade = lax.axis_index("trade")
    trades, width = values_hbm.shape
    steps = up_hbm.shape[0]
    rows = trades // n
    cols = width // LANES
    tiles = 2 if rows % (2 * SUB) == 0 else 1
    group_rows = tiles * SUB
    lat_hbm = (up_hbm, down_hbm, disc_hbm, swap_hbm, ann_hbm)

    def peer(turn):
        mask = n - 1 - turn
        if n & (n - 1):
            return lax.rem(mask + n - me + n, n)
        total, bit = 0, 1
        while bit < n:
            total = total + lax.rem(me // bit + mask // bit, 2) * bit
            bit *= 2
        return total

    def in_copy(turn):
        at = pl.ds(pl.multiple_of(peer(turn) * rows, SUB), rows)
        return pltpu.make_async_copy(values_hbm.at[at], work.at[at], in_sem.at[turn])

    lat_copies = [
        pltpu.make_async_copy(lat_hbm[i], lattice.at[i], lat_sem.at[i]) for i in range(5)
    ]
    trade_copies = [
        pltpu.make_async_copy(source, held, trade_sem.at[i])
        for i, (source, held) in enumerate(
            (
                (dates_hbm, dates_ref),
                (bucket_hbm, bucket_ref),
                (sign_hbm, sign_ref),
                (table_hbm, table_ref),
                (price_hbm, price_ref),
            )
        )
    ]
    for copy in trade_copies + lat_copies:
        copy.start()
    for turn in range(n):
        in_copy(turn).start()

    barrier = pltpu.get_barrier_semaphore()
    for k in range(1, n):
        pl.semaphore_signal(
            barrier, inc=1, device_id={"node": lax.rem(me + k, n)}, device_id_type=MESH
        )
    for k in range(1, trade_count):
        pl.semaphore_signal(
            barrier,
            inc=1,
            device_id={"trade": lax.rem(my_trade + k, trade_count)},
            device_id_type=MESH,
        )
    pl.semaphore_wait(barrier, n - 1 + trade_count - 1)

    right, left = lax.rem(me + 1, n), lax.rem(me + n - 1, n)
    first, last = pl.ds(0, LANES), pl.ds(width - LANES, LANES)
    halos = []
    for side, (target, edge) in enumerate(((right, last), (left, first))):
        for i in range(5):
            halos.append(
                pltpu.make_async_remote_copy(
                    src_ref=lat_hbm[i].at[:, edge],
                    dst_ref=halo_lattice.at[side, i],
                    send_sem=hl_send.at[side, i],
                    recv_sem=hl_recv.at[side, i],
                    device_id={"node": target},
                    device_id_type=MESH,
                )
            )
        halos.append(
            pltpu.make_async_remote_copy(
                src_ref=values_hbm.at[:, edge],
                dst_ref=halo_values.at[side],
                send_sem=hv_send.at[side],
                recv_sem=hv_recv.at[side],
                device_id={"node": target},
                device_id_type=MESH,
            )
        )
    for copy in halos:
        copy.start()

    for copy in trade_copies:
        copy.wait()
    rows_t[0:4, :] = dates_ref[...].astype(jnp.float32)
    rows_t[4:5, :] = bucket_ref[...].astype(jnp.float32)
    rows_t[5:6, :] = sign_ref[...].astype(jnp.float32)
    rows_t[6:8, :] = jnp.zeros((2, trades), jnp.float32)
    per_trade = rows_t[...].T
    levels = lax.broadcasted_iota(jnp.int32, (trades, table_ref.shape[1]), 1).astype(jnp.float32)
    strike = jnp.sum(
        jnp.where(per_trade[:, 4:5] == levels, table_ref[...], 0.0), axis=1, keepdims=True
    )
    sign = 2.0 * per_trade[:, 5:6] - 1.0
    sign_b[...] = jnp.broadcast_to(sign, (trades, LANES))
    strike_b[...] = jnp.broadcast_to(sign * strike, (trades, LANES))
    for e in range(4):
        dates_b[e] = jnp.broadcast_to(per_trade[:, e : e + 1], (trades, LANES))

    for copy in lat_copies:
        copy.wait()

    def widen(row):
        return jnp.broadcast_to(row, (SUB, LANES))

    def spread(first_step, k, up, down, disc, swap, ann):
        rows_of = (disc * up, disc * (1.0 - up - down), disc * down, ann * swap, ann)
        for i, block in enumerate(rows_of):
            for r in range(SUB):
                coef[i, first_step + r, k] = widen(block[r : r + 1])

    def prepare(k, carry):
        at = pl.ds(pl.multiple_of(k * LANES, LANES), LANES)
        for first_step in range(0, steps, SUB):
            spread(
                first_step, k, *[lattice[i, pl.ds(first_step, SUB), at] for i in range(5)]
            )
        return carry

    lax.fori_loop(0, cols, prepare, 0)

    lane = lax.broadcasted_iota(jnp.int32, (SUB, LANES), 1)
    row = lax.broadcasted_iota(jnp.int32, (SUB, LANES), 0)
    on_right = lane < LANES // 2
    has_right = jnp.where(me < n - 1, 1.0, 0.0)
    has_left = jnp.where(me > 0, 1.0, 0.0)
    inside = jnp.where(lane < steps, has_right, jnp.where(lane >= LANES - steps, has_left, 0.0))

    for copy in halos:
        copy.wait()

    for first_step in range(0, steps, SUB):
        at = pl.ds(first_step, SUB)
        up, down, disc, swap, ann = [
            jnp.where(on_right, halo_lattice[1, i, at, :], halo_lattice[0, i, at, :])
            for i in range(5)
        ]
        spread(first_step, cols, up, down, disc * inside, swap, ann * inside)

    is_first, is_last = lane == 0, lane == LANES - 1
    count = cols + 1

    def group(base, offset, total, message):
        parts = []
        for u in range(tiles):
            at = pl.ds(pl.multiple_of(base + u * SUB, SUB), SUB)
            held = [work[at, pl.ds(k * LANES, LANES)] for k in range(cols)]
            held.append(
                inside * jnp.where(on_right, halo_values[1, at, :], halo_values[0, at, :])
            )
            parts.append(held)
        dates = [
            [
                dates_b[e, pl.ds(pl.multiple_of(base + u * SUB, SUB), SUB), :]
                for e in range(4)
            ]
            for u in range(tiles)
        ]
        signs = [
            sign_b[pl.ds(pl.multiple_of(base + u * SUB, SUB), SUB), :] for u in range(tiles)
        ]
        strikes = [
            strike_b[pl.ds(pl.multiple_of(base + u * SUB, SUB), SUB), :] for u in range(tiles)
        ]

        def step_once(step, flat):
            now = step.astype(jnp.float32)
            scale, shift = [], []
            for u in range(tiles):
                d = dates[u]
                active = (d[0] == now) | (d[1] == now) | (d[2] == now) | (d[3] == now)
                scale.append(jnp.where(active, signs[u], 0.0))
                shift.append(jnp.where(active, strikes[u], 0.0))
            old = [flat[u * count : (u + 1) * count] for u in range(tiles)]
            new = [[] for _ in range(tiles)]
            for k in range(count):
                a, b, c = coef[0, step, k], coef[1, step, k], coef[2, step, k]
                pay, ann = coef[3, step, k], coef[4, step, k]
                for u in range(tiles):
                    x = old[u]
                    above = pltpu.roll(
                        jnp.where(is_first, x[(k + 1) % count], x[k]), LANES - 1, 1
                    )
                    below = pltpu.roll(jnp.where(is_last, x[k - 1], x[k]), 1, 1)
                    rolled = a * above + b * x[k] + c * below
                    new[u].append(jnp.maximum(rolled, scale[u] * pay - shift[u] * ann))
            return tuple(x for u in range(tiles) for x in new[u])

        flat = lax.fori_loop(0, steps, step_once, tuple(x for held in parts for x in held))
        for u in range(tiles):
            at = pl.ds(pl.multiple_of(base + u * SUB, SUB), SUB)
            priced = jnp.zeros((SUB, LANES), jnp.float32)
            for k in range(cols):
                x = flat[u * count + k]
                work[at, pl.ds(k * LANES, LANES)] = x
                priced = priced + x * widen(price_ref[:, pl.ds(k * LANES, LANES)])
            total = total + priced
            summed = jnp.sum(priced, axis=1, keepdims=True)
            message = message + jnp.where(lane == offset + u * SUB + row, summed, 0.0)
        return total, message

    my_cols = pl.ds(pl.multiple_of(me * width, LANES), width)

    def block_copy(turn):
        target = peer(turn)
        return pltpu.make_async_remote_copy(
            src_ref=work.at[pl.ds(pl.multiple_of(target * rows, SUB), rows)],
            dst_ref=out_ref.at[:, my_cols],
            send_sem=block_send.at[turn],
            recv_sem=block_recv.at[turn],
            device_id={"node": target},
            device_id_type=MESH,
        )

    zero = jnp.zeros((SUB, LANES), jnp.float32)

    def chunk(turn, total):
        start = peer(turn) * rows
        in_copy(turn).wait()

        def one(g, carry):
            return group(start + g * group_rows, g * group_rows, *carry)

        total, message = lax.fori_loop(0, rows // group_rows, one, (total, zero))
        msg_send[turn] = message

        @pl.when(turn < n - 1)
        def _():
            block_copy(turn).start()

        return total

    total = lax.fori_loop(0, n, chunk, zero)
    own = pltpu.make_async_copy(
        work.at[pl.ds(pl.multiple_of(me * rows, SUB), rows)], out_ref.at[:, my_cols], self_sem
    )
    own.start()

    z_send[...] = total
    z_copies = [
        pltpu.make_async_remote_copy(
            src_ref=z_send,
            dst_ref=z_recv.at[k - 1],
            send_sem=zs_sem.at[k - 1],
            recv_sem=zr_sem.at[k - 1],
            device_id={"trade": lax.rem(my_trade + k, trade_count)},
            device_id_type=MESH,
        )
        for k in range(1, trade_count)
    ]
    for copy in z_copies:
        copy.start()
    for k, copy in enumerate(z_copies):
        copy.wait()
        total = total + z_recv[k]
    summed = jnp.where(lane == LANES - 1, jnp.sum(total, axis=1, keepdims=True), 0.0)
    for turn in range(n):
        msg_send[turn] = msg_send[turn] + summed

    def msg_copy(turn):
        return pltpu.make_async_remote_copy(
            src_ref=msg_send.at[turn],
            dst_ref=msg_recv.at[turn],
            send_sem=ms_sem.at[turn],
            recv_sem=mr_sem.at[turn],
            device_id={"node": peer(turn)},
            device_id_type=MESH,
        )

    own.wait()
    for turn in range(n - 1):
        msg_copy(turn).start()
    result = msg_send[n - 1]
    for turn in range(n - 1):
        msg_copy(turn).wait()
        result = result + msg_recv[turn]
    prices = jnp.sum(result, axis=0, keepdims=True)
    small_ref[...] = prices * jnp.where(lane[:1] == LANES - 1, 1.0 / trades, 1.0)
    for turn in range(n - 1):
        block_copy(turn).wait()


def local(
    node_count,
    trade_count,
    values_in,
    prob_up,
    prob_down,
    discount,
    swap_rate,
    annuity,
    state_price,
    exercise_step,
    strike_bucket,
    notional_sign,
    strike_table,
):
    trades, width = values_in.shape
    steps = prob_up.shape[0]
    n = node_count
    rows = trades // n
    f32 = jnp.float32
    dma = pltpu.SemaphoreType.DMA
    hbm_spec = pl.BlockSpec(memory_space=pltpu.HBM)
    vmem_spec = pl.BlockSpec(memory_space=pltpu.VMEM)
    values, small = pl.pallas_call(
        functools.partial(kernel, n, trade_count),
        out_shape=(
            jax.ShapeDtypeStruct((rows, width * n), f32),
            jax.ShapeDtypeStruct((1, LANES), f32),
        ),
        in_specs=[hbm_spec] * 11,
        out_specs=(hbm_spec, vmem_spec),
        scratch_shapes=[
            pltpu.VMEM((trades, width), f32),
            pltpu.VMEM((5, steps, width), f32),
            pltpu.VMEM((1, width), f32),
            pltpu.VMEM((4, trades), jnp.int32),
            pltpu.VMEM((1, trades), jnp.int32),
            pltpu.VMEM((1, trades), jnp.int32),
            pltpu.VMEM((1, strike_table.shape[0]), f32),
            pltpu.VMEM((2, trades, LANES), f32),
            pltpu.VMEM((2, 5, steps, LANES), f32),
            pltpu.VMEM((5, steps, width // LANES + 1, SUB, LANES), f32),
            pltpu.VMEM((SUB, trades), f32),
            pltpu.VMEM((trades, LANES), f32),
            pltpu.VMEM((trades, LANES), f32),
            pltpu.VMEM((4, trades, LANES), f32),
            pltpu.VMEM((SUB, LANES), f32),
            pltpu.VMEM((trade_count - 1, SUB, LANES), f32),
            pltpu.VMEM((n, SUB, LANES), f32),
            pltpu.VMEM((n - 1, SUB, LANES), f32),
            dma((n,)),
            dma((5,)),
            dma((5,)),
            dma,
            dma((2,)),
            dma((2,)),
            dma((2, 5)),
            dma((2, 5)),
            dma((n - 1,)),
            dma((n - 1,)),
            dma((trade_count - 1,)),
            dma((trade_count - 1,)),
            dma((n - 1,)),
            dma((n - 1,)),
        ],
        compiler_params=pltpu.CompilerParams(
            collective_id=0, has_side_effects=True, vmem_limit_bytes=67043328
        ),
    )(
        values_in,
        prob_up,
        prob_down,
        discount,
        swap_rate,
        annuity,
        state_price.reshape(1, width),
        exercise_step.T,
        strike_bucket.reshape(1, trades),
        notional_sign.reshape(1, trades),
        strike_table.reshape(1, strike_table.shape[0]),
    )
    return (values, small[0, :rows], small[0, LANES - 1])


def solution(mesh):
    in_specs = (
        P("trade", "node"),
        P(None, "node"),
        P(None, "node"),
        P(None, "node"),
        P(None, "node"),
        P(None, "node"),
        P("node"),
        P("trade", None),
        P("trade"),
        P("trade"),
        P(),
    )
    out_specs = (P(("trade", "node"), None), P(("trade", "node")), P())
    body = functools.partial(local, mesh.shape["node"], mesh.shape["trade"])
    return jax.shard_map(body, mesh=mesh, in_specs=in_specs, out_specs=out_specs, check_vma=False)
```
